32 devices in a mesh: wide: 16 (over z, y, x), narrow: 2 (over core).
Axes of the slice: x: 2, y: 2, z: 4, core: 2. Of those that a mesh axis runs over, the one named last changes fastest.
Arguments:
- cand_ids: int32 [32, 2048], P(None, ('wide', 'narrow')), may hold values from 0 to 59999
- cand_request: int32 [2048], P(('wide', 'narrow')), may hold values from 0 to 1
- tables: bfloat16 [32, 1024, 256], P('wide'), may hold values from -4 to 4
- table_rows: int32 [32], P('wide'), may hold values from 256 to 1024
- width_choice: int32 [32], P('wide'), may hold values from 0 to 3
- projections: bfloat16 [32, 256, 128], P('wide'), may hold values from -0.5 to 0.5
- user_dense: bfloat16 [32, 512], P(('wide', 'narrow')), may hold values from -6 to 6
- user_weight: bfloat16 [512, 1024], replicated, may hold values from -0.25 to 0.25
- cross_down: bfloat16 [2048, 256], P('narrow'), may hold values from -0.125 to 0.125
- cross_up: bfloat16 [256, 2048], P(None, 'narrow'), may hold values from -0.375 to 0.375
- cross_bias: float32 [2048], replicated, may hold values from -3 to 3
- deep_in: bfloat16 [2048, 512], P('narrow'), may hold values from -0.125 to 0.125
- deep_mid: bfloat16 [512, 256], replicated, may hold values from -0.25 to 0.25
- head_cross: float32 [2048], replicated, may hold values from -0.125 to 0.125
- head_deep: float32 [256], replicated, may hold values from -0.375 to 0.375
Outputs:
- crossed: bfloat16 [2048, 2048], P(('wide', 'narrow'))
- scores: float32 [2048], P(('wide', 'narrow'))
The draws below stay inside these ranges and needn't reach their ends.
All inputs are finite; a program needn't handle non-finite values.
Results may differ from the reference program's by a relative error of at most 0.0072.
Values may be sent and summed in bfloat16 or wider, within the bound.
A program may use at most 64 MiB of HBM per device.

```python
import math
import jax
import jax.numpy as jnp
import numpy as np
from jax import lax

CAND_DEV = 64
TAB_DEV = 2
VOCAB = 1024
EMB = 256
PROJ = 128
SLOTS = 8
USER_DIM = 1024
UIN = 512
RANK = 256
DEEP1 = 512
DEEP2 = 256
F = 32
REQ_DEV = 2
REQUESTS = 32
ROWS_ALL = 2048
DENSE = 2048
N_WIDE = 16
N_NARROW = 2


def touch_ends(drawn, own_key, least, top_value):
    longest = drawn.shape.index(max(drawn.shape))
    spots = []
    for shift in (0, 1):
        where = [jax.random.randint(jax.random.fold_in(own_key, axis), (), 0, length) for axis, length in enumerate(drawn.shape)]
        where[longest] = (where[longest] + shift) % drawn.shape[longest]
        spots.append(tuple(where))
    return drawn.at[spots[0]].set(least).at[spots[1]].set(top_value)


def steps_of(stream_key, shape, shards, least, high):
    def one(dim, parts):
        heights = jax.random.uniform(jax.random.fold_in(jax.random.fold_in(stream_key, 6), dim), (parts,), jnp.float32, least / len(shards), high / len(shards))
        return jnp.repeat(jnp.exp(heights), shape[dim] // parts).reshape((-1,) + (1,) * (len(shape) - dim - 1))

    level = one(*shards[0])
    for cut in shards[1:]:
        level = level * one(*cut)
    return level


def cumulative_ranks(amount, slope):
    loads = [(1 << 20) // math.isqrt(grade ** slope) + 1 for grade in range(1, amount + 1)]
    scale = 1 + sum(loads) // (1 << 30)
    return np.cumsum(np.array([max(1, weight // scale) for weight in loads]))


def ranked_ids(stream_key, extent, count, skew):
    table = cumulative_ranks(count, skew)
    lot = jax.random.randint(jax.random.fold_in(stream_key, 1), extent, 0, int(table[count - 1]))
    standing = jnp.searchsorted(jnp.asarray(table, jnp.int32), lot, side="right")
    return jax.random.permutation(jax.random.fold_in(stream_key, 2), count)[standing].astype(jnp.int32)


def gaussian(stream_key, dims, deviation, reach, cuts=(), kind=jnp.bfloat16):
    entries = deviation * jax.random.normal(stream_key, dims, jnp.float32)
    if cuts:
        entries = entries * steps_of(stream_key, dims, cuts, -0.22, 0.18)
    return jnp.clip(entries, -reach, reach).astype(kind)


def setup_inputs(seed: int = 0) -> dict:
    key_of = jax.random.split(jax.random.key(seed), 16)
    return {
        "cand_ids": touch_ends(ranked_ids(key_of[0], (F, ROWS_ALL), 60000, 2), jax.random.fold_in(key_of[0], 3), 0, 59999).astype(jnp.int32),
        "cand_request": touch_ends(ranked_ids(key_of[1], (ROWS_ALL,), REQ_DEV, 2), jax.random.fold_in(key_of[1], 3), 0, REQ_DEV - 1).astype(jnp.int32),
        "tables": gaussian(key_of[2], (F, VOCAB, EMB), 0.3, 4.0, ((0, 16),)),
        "table_rows": touch_ends(jax.random.randint(key_of[3], (F,), VOCAB // 4, VOCAB + 1), jax.random.fold_in(key_of[3], 1), VOCAB // 4, VOCAB).astype(jnp.int32),
        "width_choice": touch_ends(jax.random.randint(key_of[4], (F,), 0, 4), jax.random.fold_in(key_of[4], 1), 0, 3).astype(jnp.int32),
        "projections": gaussian(key_of[5], (F, EMB, PROJ), PROJ ** -0.5, 0.5, ((0, 16),)),
        "user_dense": gaussian(key_of[6], (REQUESTS, UIN), 1.0, 6.0, ((0, 32),)),
        "user_weight": gaussian(key_of[7], (UIN, USER_DIM), UIN ** -0.5, 0.25),
        "cross_down": gaussian(key_of[8], (DENSE, RANK), DENSE ** -0.5, 0.125, ((0, 2),)),
        "cross_up": gaussian(key_of[9], (RANK, DENSE), RANK ** -0.5, 0.375, ((1, 2),)),
        "cross_bias": gaussian(key_of[10], (DENSE,), 0.5, 3.0, (), jnp.float32),
        "deep_in": gaussian(key_of[11], (DENSE, DEEP1), DENSE ** -0.5, 0.125, ((0, 2),)),
        "deep_mid": gaussian(key_of[12], (DEEP1, DEEP2), DEEP1 ** -0.5, 0.25),
        "head_cross": gaussian(key_of[13], (DENSE,), DENSE ** -0.5, 0.125, (), jnp.float32),
        "head_deep": gaussian(key_of[14], (DEEP2,), DEEP2 ** -0.5, 0.375, (), jnp.float32),
    }


def table_embed(t, cand_ids, tables, table_rows, width_choice, projections):
    columns = jnp.arange(EMB, dtype=jnp.int32)
    width = jnp.left_shift(jnp.int32(32), width_choice[t])
    masked = jnp.where(columns[None, :] < width, tables[t], jnp.zeros((), jnp.bfloat16))
    projected = jnp.dot(masked, projections[t], preferred_element_type=jnp.float32).astype(jnp.bfloat16)
    index = jnp.remainder(cand_ids[t], table_rows[t]).astype(jnp.int32)
    return jnp.take(projected, index, axis=0)


def dense_block(x0, cross_down, cross_up, cross_bias, deep_in, deep_mid, head_cross, head_deep):
    low = jnp.dot(x0, cross_down, preferred_element_type=jnp.float32).astype(jnp.bfloat16)
    deep = jax.nn.relu(jnp.dot(x0, deep_in, preferred_element_type=jnp.float32)).astype(jnp.bfloat16)
    upward = jnp.dot(low, cross_up, preferred_element_type=jnp.float32)
    wide_x = x0.astype(jnp.float32)
    crossed = (wide_x * (upward + cross_bias) + wide_x).astype(jnp.bfloat16)
    hidden = jax.nn.relu(jnp.dot(deep, deep_mid, preferred_element_type=jnp.float32))
    scores = jnp.dot(crossed.astype(jnp.float32), head_cross, precision=lax.Precision.HIGHEST)
    scores = scores + jnp.dot(hidden, head_deep, precision=lax.Precision.HIGHEST)
    return crossed, scores


def reference(cand_ids, cand_request, tables, table_rows, width_choice, projections, user_dense, user_weight, cross_down, cross_up, cross_bias, deep_in, deep_mid, head_cross, head_deep):
    def owner_sum(owner):
        total = jnp.zeros((ROWS_ALL, PROJ), jnp.float32)
        for k in range(TAB_DEV):
            total = total + table_embed(owner * TAB_DEV + k, cand_ids, tables, table_rows, width_choice, projections).astype(jnp.float32)
        return total.astype(jnp.bfloat16)

    def group_step(group, slots):
        for s in range(SLOTS):
            slots = slots.at[s].add(owner_sum(group * SLOTS + s).astype(jnp.float32))
        return slots

    slots = lax.fori_loop(0, N_WIDE // SLOTS, group_step, jnp.zeros((SLOTS, ROWS_ALL, PROJ), jnp.float32))
    item = slots.astype(jnp.bfloat16).transpose(1, 0, 2).reshape(ROWS_ALL, SLOTS * PROJ)
    user_vec = jax.nn.silu(jnp.dot(user_dense, user_weight, preferred_element_type=jnp.float32)).astype(jnp.bfloat16)
    positions = jnp.arange(ROWS_ALL, dtype=jnp.int32)
    request = (positions // (CAND_DEV * N_NARROW)) * REQ_DEV + cand_request
    user_part = jnp.take(user_vec, request.astype(jnp.int32), axis=0)
    x0 = jnp.concatenate([user_part, item], axis=1)
    blocks = x0.reshape(N_WIDE, ROWS_ALL // N_WIDE, DENSE)

    def run(block):
        return dense_block(block, cross_down, cross_up, cross_bias, deep_in, deep_mid, head_cross, head_deep)

    crossed, scores = lax.map(run, blocks)
    return crossed.reshape(ROWS_ALL, DENSE), scores.reshape(ROWS_ALL)
```

```python
import functools

import jax
import jax.numpy as jnp
from jax import lax
from jax.experimental import pallas as pl
from jax.experimental.pallas import tpu as pltpu
from jax.sharding import PartitionSpec as P

GROUP = 4
F32 = jnp.float32
BF16 = jnp.bfloat16


def dot(a, b):
    return jnp.dot(a, b, preferred_element_type=F32)


def row_to_column(row, eye):
    return jnp.sum(jnp.where(eye, row, 0.0), axis=1, keepdims=True)


def kernel(
    nw,
    nn,
    ids_in,
    request_in,
    tables_in,
    rows_in,
    choice_in,
    proj_in,
    dense_in,
    user_weight_in,
    down_in,
    up_in,
    bias_in,
    deep_in,
    mid_in,
    head_cross_in,
    head_deep_in,
    crossed_out,
    scores_out,
    ids,
    request,
    tables,
    rows,
    choice,
    proj,
    dense,
    user_weight,
    down,
    up,
    bias,
    deep_w,
    mid,
    head_cross,
    head_deep,
    ids_send,
    ids_recv,
    projected,
    onehot,
    emb_send,
    emb_recv,
    x0,
    crossed,
    scores,
    local_sem,
    out_sem,
    ids_ssem,
    ids_rsem,
    emb_ssem,
    emb_rsem,
    nar_ssem,
    nar_rsem,
):
    me = lax.axis_index("wide")
    core = lax.axis_index("narrow")
    tab_dev, vocab, emb_width = tables.shape
    cand = request.shape[1]
    width = projected.shape[1]
    total = bias.shape[1]
    user_dim = user_weight.shape[1]
    req_dev = dense.shape[1]
    block = down.shape[1]
    column_block = up.shape[2]

    loads = {}
    for at, (name, source, target) in enumerate(
        (
            ("ids", ids_in, ids),
            ("proj", proj_in, proj),
            ("choice", choice_in, choice),
            ("rows", rows_in, rows),
            ("tables", tables_in, tables),
            ("dense", dense_in, dense.at[core]),
            ("request", request_in, request),
            ("user_weight", user_weight_in, user_weight),
            ("down", down_in, down.at[core]),
            ("deep", deep_in, deep_w.at[core]),
            ("up", up_in, up.at[core]),
            ("mid", mid_in, mid),
            ("bias", bias_in, bias),
            ("head_cross", head_cross_in, head_cross),
            ("head_deep", head_deep_in, head_deep),
        )
    ):
        loads[name] = pltpu.make_async_copy(source, target, local_sem.at[at])
        loads[name].start()

    barrier = pltpu.get_barrier_semaphore()

    def peer_of(j):
        return lax.rem(me + nw // 2 + (j // 2) * (1 - 2 * (j % 2)) - (j % 2) + nw, nw)

    def greet(j, carry):
        pl.semaphore_signal(
            barrier, inc=1, device_id={"wide": peer_of(j)}, device_id_type=pl.DeviceIdType.MESH
        )
        return carry

    lax.fori_loop(0, nw - 1, greet, 0, unroll=nw <= 16)
    for step in range(1, nn):
        pl.semaphore_signal(
            barrier,
            inc=1,
            device_id={"narrow": lax.rem(core + step, nn)},
            device_id_type=pl.DeviceIdType.MESH,
        )

    loads["ids"].wait()
    for o in range(nw):
        ids_send[o] = ids[o * tab_dev : (o + 1) * tab_dev, :]
    ids_recv[me] = ids_send[me]

    loads["proj"].wait()
    loads["choice"].wait()
    loads["tables"].wait()
    row_index = lax.broadcasted_iota(jnp.int32, (emb_width, width), 0)
    for t in range(tab_dev):
        kept = jnp.left_shift(jnp.full((1, 1), 32, jnp.int32), choice[:, t : t + 1])
        used = jnp.where(row_index < kept, proj[t].astype(F32), 0.0).astype(BF16)
        projected[t * vocab : (t + 1) * vocab, :] = dot(tables[t], used).astype(BF16)

    pl.semaphore_wait(barrier, nw - 1 + nn - 1)

    def ids_copy(to, index):
        return pltpu.make_async_remote_copy(
            src_ref=ids_send.at[to],
            dst_ref=ids_recv.at[index],
            send_sem=ids_ssem.at[to],
            recv_sem=ids_rsem.at[index],
            device_id={"wide": to},
            device_id_type=pl.DeviceIdType.MESH,
        )

    def emb_copy(to, index):
        return pltpu.make_async_remote_copy(
            src_ref=emb_send.at[to],
            dst_ref=emb_recv.at[index],
            send_sem=emb_ssem.at[to],
            recv_sem=emb_rsem.at[index],
            device_id={"wide": to},
            device_id_type=pl.DeviceIdType.MESH,
        )

    def narrow_copy(kind, to, index):
        source, target = (
            (dense_in, dense),
            (down_in, down),
            (deep_in, deep_w),
            (up_in, up),
        )[kind]
        return pltpu.make_async_remote_copy(
            src_ref=source,
            dst_ref=target.at[index],
            send_sem=nar_ssem.at[kind, to],
            recv_sem=nar_rsem.at[kind, index],
            device_id={"narrow": to},
            device_id_type=pl.DeviceIdType.MESH,
        )

    def send_ids(j, carry):
        ids_copy(peer_of(j), me).start()
        return carry

    lax.fori_loop(0, nw - 1, send_ids, 0, unroll=nw <= 16)
    for kind in range(4):
        for step in range(1, nn):
            narrow_copy(kind, lax.rem(core + step, nn), core).start()

    eye = lax.broadcasted_iota(jnp.int32, (cand, cand), 0) == lax.broadcasted_iota(
        jnp.int32, (cand, cand), 1
    )
    for name in ("request", "user_weight", "dense", "rows"):
        loads[name].wait()
    wanted = row_to_column(request[...].astype(F32), eye)
    for step in range(1, nn):
        narrow_copy(0, core, lax.rem(core + step, nn)).wait_recv()
    chosen = jnp.zeros((cand, dense.shape[2]), F32)
    for n in range(nn):
        for r in range(req_dev):
            chosen = jnp.where(
                wanted == float(n * req_dev + r), dense[n, r : r + 1, :].astype(F32), chosen
            )
    x0[:, :user_dim] = jax.nn.silu(dot(chosen.astype(BF16), user_weight[...])).astype(BF16)

    limit = rows[...].astype(F32)
    inverse = 1.0 / limit
    lane = lax.broadcasted_iota(jnp.int32, (cand, vocab), 1).astype(F32)

    def look_up(group, last):
        for i in range(GROUP):
            j = group * GROUP + i
            peer = peer_of(j)
            if not (last and i == GROUP - 1):
                ids_copy(me, peer).wait_recv()
            values = ids_recv[peer].astype(F32)
            for t in range(tab_dev):
                value = values[t : t + 1, :]
                most = limit[:, t : t + 1]
                index = value - jnp.floor(value * inverse[:, t : t + 1]) * most
                index = jnp.where(index < 0.0, index + most, index)
                index = jnp.where(index >= most, index - most, index)
                onehot[i * cand : (i + 1) * cand, t * vocab : (t + 1) * vocab] = jnp.where(
                    row_to_column(index, eye) == lane, 1.0, 0.0
                ).astype(BF16)
        pooled = dot(onehot[...], projected[...]).astype(BF16)
        for i in range(GROUP):
            j = group * GROUP + i
            part = pooled[i * cand : (i + 1) * cand]
            if last and i == GROUP - 1:
                emb_recv[me] = part
            else:
                peer = peer_of(j)
                emb_send[peer] = part
                emb_copy(peer, me).start()

    groups = nw // GROUP

    def look_up_loop(group, carry):
        look_up(group, False)
        return carry

    lax.fori_loop(0, groups - 1, look_up_loop, 0)
    look_up(groups - 1, True)

    for name in ("down", "deep"):
        loads[name].wait()
    for kind in (1, 2):
        for step in range(1, nn):
            narrow_copy(kind, core, lax.rem(core + step, nn)).wait_recv()
    low = jnp.zeros((cand, down.shape[2]), F32)
    deep = jnp.zeros((cand, deep_w.shape[2]), F32)
    for n in range(user_dim // block):
        part = x0[:, n * block : (n + 1) * block]
        low = low + dot(part, down[n])
        deep = deep + dot(part, deep_w[n])

    for name in ("up", "mid", "bias", "head_cross", "head_deep"):
        loads[name].wait()
    for step in range(1, nn):
        narrow_copy(3, core, lax.rem(core + step, nn)).wait_recv()

    def wait_emb(j, carry):
        emb_copy(me, peer_of(nw - 2 - j)).wait_recv()
        return carry

    lax.fori_loop(0, nw - 1, wait_emb, 0, unroll=nw <= 16)
    slots = (total - user_dim) // width
    for s in range(slots):
        item = emb_recv[s].astype(F32)
        for g in range(1, nw // slots):
            item = item + emb_recv[g * slots + s].astype(F32)
        x0[:, user_dim + s * width : user_dim + (s + 1) * width] = item.astype(BF16)
    for n in range(user_dim // block, total // block):
        part = x0[:, n * block : (n + 1) * block]
        low = low + dot(part, down[n])
        deep = deep + dot(part, deep_w[n])
    low = low.astype(BF16)
    deep = jax.nn.relu(deep).astype(BF16)
    score = jnp.zeros((cand, 1), F32)
    stores = []
    for n in range(nn):
        span = slice(n * column_block, (n + 1) * column_block)
        base = x0[:, span].astype(F32)
        out = (base * (dot(low, up[n]) + bias[:, span]) + base).astype(BF16)
        crossed[:, span] = out
        stores.append(pltpu.make_async_copy(crossed.at[:, span], crossed_out.at[:, span], out_sem.at[n]))
        stores[-1].start()
        score = score + jnp.sum(out.astype(F32) * head_cross[:, span], axis=1, keepdims=True)
    hidden = jax.nn.relu(dot(deep, mid[...]))
    score = score + jnp.sum(hidden * head_deep[...], axis=1, keepdims=True)
    scores[...] = jnp.sum(jnp.where(eye, score, 0.0), axis=0, keepdims=True)
    stores.append(pltpu.make_async_copy(scores, scores_out, out_sem.at[nn]))
    stores[-1].start()

    def drain(j, carry):
        ids_copy(peer_of(j), me).wait_send()
        emb_copy(peer_of(j), me).wait_send()
        return carry

    lax.fori_loop(0, nw - 1, drain, 0, unroll=nw <= 16)
    for kind in range(4):
        for step in range(1, nn):
            narrow_copy(kind, lax.rem(core + step, nn), core).wait_send()
    for store in stores:
        store.wait()


def per_device(
    cand_ids,
    cand_request,
    tables,
    table_rows,
    width_choice,
    projections,
    user_dense,
    user_weight,
    cross_down,
    cross_up,
    cross_bias,
    deep_in,
    deep_mid,
    head_cross,
    head_deep,
):
    nw = lax.axis_size("wide")
    nn = lax.axis_size("narrow")
    cand = cand_request.shape[0]
    tab_dev, vocab, emb_width = tables.shape
    width = projections.shape[2]
    total = cross_bias.shape[0]
    operands = (
        cand_ids,
        cand_request.reshape(1, -1),
        tables,
        table_rows.reshape(1, -1),
        width_choice.reshape(1, -1),
        projections,
        user_dense,
        user_weight,
        cross_down,
        cross_up,
        cross_bias.reshape(1, -1),
        deep_in,
        deep_mid,
        head_cross.reshape(1, -1),
        head_deep.reshape(1, -1),
    )
    gathered = (6, 8, 9, 11)
    scratch = [
        pltpu.VMEM(((nn,) if at in gathered else ()) + a.shape, a.dtype)
        for at, a in enumerate(operands)
    ]
    scratch += [
        pltpu.VMEM((nw, tab_dev, cand), jnp.int32),
        pltpu.VMEM((nw, tab_dev, cand), jnp.int32),
        pltpu.VMEM((tab_dev * vocab, width), BF16),
        pltpu.VMEM((GROUP * cand, tab_dev * vocab), BF16),
        pltpu.VMEM((nw, cand, width), BF16),
        pltpu.VMEM((nw, cand, width), BF16),
        pltpu.VMEM((cand, total), BF16),
        pltpu.VMEM((cand, total), BF16),
        pltpu.VMEM((1, cand), F32),
        pltpu.SemaphoreType.DMA((len(operands),)),
        pltpu.SemaphoreType.DMA((nn + 1,)),
        pltpu.SemaphoreType.DMA((nw,)),
        pltpu.SemaphoreType.DMA((nw,)),
        pltpu.SemaphoreType.DMA((nw,)),
        pltpu.SemaphoreType.DMA((nw,)),
        pltpu.SemaphoreType.DMA((4, nn)),
        pltpu.SemaphoreType.DMA((4, nn)),
    ]
    crossed, scores = pl.pallas_call(
        functools.partial(kernel, nw, nn),
        out_shape=(
            jax.ShapeDtypeStruct((cand, total), BF16),
            jax.ShapeDtypeStruct((1, cand), F32),
        ),
        in_specs=[pl.BlockSpec(memory_space=pl.ANY)] * len(operands),
        out_specs=(pl.BlockSpec(memory_space=pl.ANY), pl.BlockSpec(memory_space=pl.ANY)),
        scratch_shapes=scratch,
        compiler_params=pltpu.CompilerParams(
            collective_id=0, has_side_effects=True, vmem_limit_bytes=48 * 1024 * 1024
        ),
        name="score",
    )(*operands)
    return crossed, scores.reshape(cand)


def solution(mesh):
    return jax.shard_map(
        per_device,
        mesh=mesh,
        in_specs=(
            P(None, ("wide", "narrow")),
            P(("wide", "narrow")),
            P("wide", None, None),
            P("wide"),
            P("wide"),
            P("wide", None, None),
            P(("wide", "narrow"), None),
            P(),
            P("narrow", None),
            P(None, "narrow"),
            P(),
            P("narrow", None),
            P(),
            P(),
            P(),
        ),
        out_specs=(P(("wide", "narrow"), None), P(("wide", "narrow"))),
        check_vma=False,
    )
```

```python
import functools

import jax
import jax.numpy as jnp
from jax import lax
from jax.experimental import pallas as pl
from jax.experimental.pallas import tpu as pltpu
from jax.sharding import PartitionSpec as P

GROUP = 4
SPLIT = 4
PLANES = 4
F32 = jnp.float32
BF16 = jnp.bfloat16


def dot(a, b):
    return jnp.dot(a, b, preferred_element_type=F32)


def row_to_column(row, eye):
    return jnp.sum(jnp.where(eye, row, 0.0), axis=1, keepdims=True)


def kernel(
    nw,
    nn,
    ids_in,
    request_in,
    tables_in,
    rows_in,
    choice_in,
    proj_in,
    dense_in,
    user_weight_in,
    down_in,
    up_in,
    bias_in,
    deep_in,
    mid_in,
    head_cross_in,
    head_deep_in,
    crossed_out,
    scores_out,
    ids,
    request,
    tables,
    rows,
    choice,
    proj,
    dense,
    user_weight,
    down,
    up,
    bias,
    deep_w,
    mid,
    head_cross,
    head_deep,
    ids_send,
    ids_recv,
    projected,
    onehot,
    emb_send,
    emb_recv,
    x0,
    crossed,
    scores,
    local_sem,
    out_sem,
    ids_ssem,
    ids_rsem,
    emb_ssem,
    emb_rsem,
    nar_ssem,
    nar_rsem,
):
    me = lax.axis_index("wide")
    core = lax.axis_index("narrow")
    tab_dev, vocab, emb_width = tables.shape
    cand = request.shape[1]
    part_rows = projected.shape[1]
    width = projected.shape[2] // SPLIT
    total = bias.shape[1]
    user_dim = user_weight.shape[1]
    req_dev = dense.shape[1]
    block = down.shape[1]
    column_block = up.shape[2]

    loads = {}
    for at, (name, source, target) in enumerate(
        (
            ("ids", ids_in, ids),
            ("proj", proj_in, proj),
            ("choice", choice_in, choice),
            ("rows", rows_in, rows),
            ("tables", tables_in, tables),
            ("dense", dense_in, dense.at[core]),
            ("request", request_in, request),
            ("user_weight", user_weight_in, user_weight),
            ("down", down_in, down.at[core]),
            ("deep", deep_in, deep_w.at[core]),
            ("up", up_in, up.at[core]),
            ("mid", mid_in, mid),
            ("bias", bias_in, bias),
            ("head_cross", head_cross_in, head_cross),
            ("head_deep", head_deep_in, head_deep),
        )
    ):
        loads[name] = pltpu.make_async_copy(source, target, local_sem.at[at])
        loads[name].start()

    barrier = pltpu.get_barrier_semaphore()

    plane_size = nw // PLANES
    my_plane = me // plane_size
    my_half = my_plane // 2
    planes = (2 - my_half, 3 - 3 * my_half, my_half * 2 + 1 - my_plane % 2, my_plane)

    def peer_at(order, i):
        return planes[order] * plane_size + (me + i + 1) % plane_size

    def each_peer(do):
        for order in range(PLANES):

            def step(i, carry, order=order):
                do(peer_at(order, i))
                return carry

            lax.fori_loop(0, plane_size - (order == PLANES - 1), step, 0, unroll=nw <= 16)

    def greet(peer):
        pl.semaphore_signal(
            barrier, inc=1, device_id={"wide": peer}, device_id_type=pl.DeviceIdType.MESH
        )

    each_peer(greet)
    for step in range(1, nn):
        pl.semaphore_signal(
            barrier,
            inc=1,
            device_id={"narrow": lax.rem(core + step, nn)},
            device_id_type=pl.DeviceIdType.MESH,
        )

    loads["ids"].wait()
    for o in range(nw):
        ids_send[o] = ids[o * tab_dev : (o + 1) * tab_dev, :]
    ids_recv[me] = ids_send[me]

    loads["proj"].wait()
    loads["choice"].wait()
    loads["tables"].wait()
    row_index = lax.broadcasted_iota(jnp.int32, (emb_width, width), 0)
    for t in range(tab_dev):
        kept = jnp.left_shift(jnp.full((1, 1), 32, jnp.int32), choice[:, t : t + 1])
        used = jnp.where(row_index < kept, proj[t].astype(F32), 0.0).astype(BF16)
        for h in range(SPLIT):
            projected[t, :, h * width : (h + 1) * width] = dot(
                tables[t, h * part_rows : (h + 1) * part_rows, :], used
            ).astype(BF16)

    pl.semaphore_wait(barrier, nw - 1 + nn - 1)

    def ids_copy(to, index):
        return pltpu.make_async_remote_copy(
            src_ref=ids_send.at[to],
            dst_ref=ids_recv.at[index],
            send_sem=ids_ssem.at[to],
            recv_sem=ids_rsem.at[index],
            device_id={"wide": to},
            device_id_type=pl.DeviceIdType.MESH,
        )

    def emb_copy(to, index):
        return pltpu.make_async_remote_copy(
            src_ref=emb_send.at[to],
            dst_ref=emb_recv.at[index],
            send_sem=emb_ssem.at[to],
            recv_sem=emb_rsem.at[index],
            device_id={"wide": to},
            device_id_type=pl.DeviceIdType.MESH,
        )

    def narrow_copy(kind, to, index):
        source, target = (
            (dense_in, dense),
            (down_in, down),
            (deep_in, deep_w),
            (up_in, up),
        )[kind]
        return pltpu.make_async_remote_copy(
            src_ref=source,
            dst_ref=target.at[index],
            send_sem=nar_ssem.at[kind, to],
            recv_sem=nar_rsem.at[kind, index],
            device_id={"narrow": to},
            device_id_type=pl.DeviceIdType.MESH,
        )

    each_peer(lambda peer: ids_copy(peer, me).start())
    for kind in range(4):
        for step in range(1, nn):
            narrow_copy(kind, lax.rem(core + step, nn), core).start()

    eye = lax.broadcasted_iota(jnp.int32, (cand, cand), 0) == lax.broadcasted_iota(
        jnp.int32, (cand, cand), 1
    )
    for name in ("request", "user_weight", "dense", "rows"):
        loads[name].wait()
    wanted = row_to_column(request[...].astype(F32), eye)
    for step in range(1, nn):
        narrow_copy(0, core, lax.rem(core + step, nn)).wait_recv()
    chosen = jnp.zeros((cand, dense.shape[2]), F32)
    for n in range(nn):
        for r in range(req_dev):
            chosen = jnp.where(
                wanted == float(n * req_dev + r), dense[n, r : r + 1, :].astype(F32), chosen
            )
    x0[:, :user_dim] = jax.nn.silu(dot(chosen.astype(BF16), user_weight[...])).astype(BF16)

    limit = rows[...].astype(F32)
    inverse = 1.0 / limit
    lane = lax.broadcasted_iota(jnp.int32, (cand, part_rows), 1).astype(F32)

    def look_up(order, group, last):
        highs = []
        for i in range(GROUP):
            peer = peer_at(order, group * GROUP + i)
            if not (last and i == GROUP - 1):
                ids_copy(me, peer).wait_recv()
            values = ids_recv[peer].astype(F32)
            for t in range(tab_dev):
                value = values[t : t + 1, :]
                most = limit[:, t : t + 1]
                index = value - jnp.floor(value * inverse[:, t : t + 1]) * most
                index = jnp.where(index < 0.0, index + most, index)
                index = jnp.where(index >= most, index - most, index)
                high = sum(
                    jnp.where(index >= float(h * part_rows), 1.0, 0.0) for h in range(1, SPLIT)
                )
                low_index = row_to_column(index - high * float(part_rows), eye)
                highs.append(row_to_column(high, eye))
                onehot[t, i * cand : (i + 1) * cand, :] = jnp.where(
                    low_index == lane, 1.0, 0.0
                ).astype(BF16)
        found = [dot(onehot[t], projected[t]) for t in range(tab_dev)]
        for i in range(GROUP):
            total_rows = jnp.zeros((cand, width), F32)
            for t in range(tab_dev):
                high = highs[i * tab_dev + t]
                for h in range(SPLIT):
                    piece = found[t][i * cand : (i + 1) * cand, h * width : (h + 1) * width]
                    total_rows = total_rows + jnp.where(high == float(h), piece, 0.0)
            part = total_rows.astype(BF16)
            if last and i == GROUP - 1:
                emb_recv[me] = part
            else:
                peer = peer_at(order, group * GROUP + i)
                emb_send[peer] = part
                emb_copy(peer, me).start()

    groups = plane_size // GROUP
    for order in range(PLANES):
        final = order == PLANES - 1

        def look_up_loop(group, carry, order=order):
            look_up(order, group, False)
            return carry

        if groups - final > 1:
            lax.fori_loop(0, groups - final, look_up_loop, 0)
        elif groups - final == 1:
            look_up(order, 0, False)
        if final:
            look_up(order, groups - 1, True)

    for name in ("down", "deep"):
        loads[name].wait()
    for kind in (1, 2):
        for step in range(1, nn):
            narrow_copy(kind, core, lax.rem(core + step, nn)).wait_recv()
    low = jnp.zeros((cand, down.shape[2]), F32)
    deep = jnp.zeros((cand, deep_w.shape[2]), F32)
    for n in range(user_dim // block):
        part = x0[:, n * block : (n + 1) * block]
        low = low + dot(part, down[n])
        deep = deep + dot(part, deep_w[n])

    for name in ("up", "mid", "bias", "head_cross", "head_deep"):
        loads[name].wait()
    for step in range(1, nn):
        narrow_copy(3, core, lax.rem(core + step, nn)).wait_recv()

    each_peer(lambda peer: emb_copy(me, peer).wait_recv())
    slots = (total - user_dim) // width
    for s in range(slots):
        item = emb_recv[s].astype(F32)
        for g in range(1, nw // slots):
            item = item + emb_recv[g * slots + s].astype(F32)
        x0[:, user_dim + s * width : user_dim + (s + 1) * width] = item.astype(BF16)
    for n in range(user_dim // block, total // block):
        part = x0[:, n * block : (n + 1) * block]
        low = low + dot(part, down[n])
        deep = deep + dot(part, deep_w[n])
    low = low.astype(BF16)
    deep = jax.nn.relu(deep).astype(BF16)
    score = jnp.zeros((cand, 1), F32)
    stores = []
    for n in range(nn):
        span = slice(n * column_block, (n + 1) * column_block)
        base = x0[:, span].astype(F32)
        out = (base * (dot(low, up[n]) + bias[:, span]) + base).astype(BF16)
        crossed[:, span] = out
        stores.append(pltpu.make_async_copy(crossed.at[:, span], crossed_out.at[:, span], out_sem.at[n]))
        stores[-1].start()
        score = score + jnp.sum(out.astype(F32) * head_cross[:, span], axis=1, keepdims=True)
    hidden = jax.nn.relu(dot(deep, mid[...]))
    score = score + jnp.sum(hidden * head_deep[...], axis=1, keepdims=True)
    scores[...] = jnp.sum(jnp.where(eye, score, 0.0), axis=0, keepdims=True)
    stores.append(pltpu.make_async_copy(scores, scores_out, out_sem.at[nn]))
    stores[-1].start()

    def drain(peer):
        ids_copy(peer, me).wait_send()
        emb_copy(peer, me).wait_send()

    each_peer(drain)
    for kind in range(4):
        for step in range(1, nn):
            narrow_copy(kind, lax.rem(core + step, nn), core).wait_send()
    for store in stores:
        store.wait()


def per_device(
    cand_ids,
    cand_request,
    tables,
    table_rows,
    width_choice,
    projections,
    user_dense,
    user_weight,
    cross_down,
    cross_up,
    cross_bias,
    deep_in,
    deep_mid,
    head_cross,
    head_deep,
):
    nw = lax.axis_size("wide")
    nn = lax.axis_size("narrow")
    cand = cand_request.shape[0]
    tab_dev, vocab, emb_width = tables.shape
    width = projections.shape[2]
    total = cross_bias.shape[0]
    operands = (
        cand_ids,
        cand_request.reshape(1, -1),
        tables,
        table_rows.reshape(1, -1),
        width_choice.reshape(1, -1),
        projections,
        user_dense,
        user_weight,
        cross_down,
        cross_up,
        cross_bias.reshape(1, -1),
        deep_in,
        deep_mid,
        head_cross.reshape(1, -1),
        head_deep.reshape(1, -1),
    )
    gathered = (6, 8, 9, 11)
    scratch = [
        pltpu.VMEM(((nn,) if at in gathered else ()) + a.shape, a.dtype)
        for at, a in enumerate(operands)
    ]
    scratch += [
        pltpu.VMEM((nw, tab_dev, cand), jnp.int32),
        pltpu.VMEM((nw, tab_dev, cand), jnp.int32),
        pltpu.VMEM((tab_dev, vocab // SPLIT, SPLIT * width), BF16),
        pltpu.VMEM((tab_dev, GROUP * cand, vocab // SPLIT), BF16),
        pltpu.VMEM((nw, cand, width), BF16),
        pltpu.VMEM((nw, cand, width), BF16),
        pltpu.VMEM((cand, total), BF16),
        pltpu.VMEM((cand, total), BF16),
        pltpu.VMEM((1, cand), F32),
        pltpu.SemaphoreType.DMA((len(operands),)),
        pltpu.SemaphoreType.DMA((nn + 1,)),
        pltpu.SemaphoreType.DMA((nw,)),
        pltpu.SemaphoreType.DMA((nw,)),
        pltpu.SemaphoreType.DMA((nw,)),
        pltpu.SemaphoreType.DMA((nw,)),
        pltpu.SemaphoreType.DMA((4, nn)),
        pltpu.SemaphoreType.DMA((4, nn)),
    ]
    crossed, scores = pl.pallas_call(
        functools.partial(kernel, nw, nn),
        out_shape=(
            jax.ShapeDtypeStruct((cand, total), BF16),
            jax.ShapeDtypeStruct((1, cand), F32),
        ),
        in_specs=[pl.BlockSpec(memory_space=pl.ANY)] * len(operands),
        out_specs=(pl.BlockSpec(memory_space=pl.ANY), pl.BlockSpec(memory_space=pl.ANY)),
        scratch_shapes=scratch,
        compiler_params=pltpu.CompilerParams(
            collective_id=0, has_side_effects=True, vmem_limit_bytes=67043328
        ),
        name="score",
    )(*operands)
    return crossed, scores.reshape(cand)


def solution(mesh):
    return jax.shard_map(
        per_device,
        mesh=mesh,
        in_specs=(
            P(None, ("wide", "narrow")),
            P(("wide", "narrow")),
            P("wide", None, None),
            P("wide"),
            P("wide"),
            P("wide", None, None),
            P(("wide", "narrow"), None),
            P(),
            P("narrow", None),
            P(None, "narrow"),
            P(),
            P("narrow", None),
            P(),
            P(),
            P(),
        ),
        out_specs=(P(("wide", "narrow"), None), P(("wide", "narrow"))),
        check_vma=False,
    )
```

```python
import functools

import jax
import jax.numpy as jnp
from jax import lax
from jax.experimental import pallas as pl
from jax.experimental.pallas import tpu as pltpu
from jax.sharding import PartitionSpec as P

GROUP = 4
SPLIT = 4
PLANES = 4
F32 = jnp.float32
BF16 = jnp.bfloat16


def dot(a, b):
    return jnp.dot(a, b, preferred_element_type=F32)


def row_to_column(row, eye):
    return jnp.sum(jnp.where(eye, row, 0.0), axis=1, keepdims=True)


def kernel(
    nw,
    nn,
    ids_in,
    request_in,
    tables_in,
    rows_in,
    choice_in,
    proj_in,
    dense_in,
    user_weight_in,
    down_in,
    up_in,
    bias_in,
    deep_in,
    mid_in,
    head_cross_in,
    head_deep_in,
    crossed,
    scores,
    ids,
    request,
    tables,
    rows,
    choice,
    proj,
    dense,
    user_weight,
    down,
    up,
    bias,
    deep_w,
    mid,
    head_cross,
    head_deep,
    ids_send,
    ids_recv,
    projected,
    onehot,
    emb_send,
    emb_recv,
    x0,
    local_sem,
    ids_ssem,
    ids_rsem,
    emb_ssem,
    emb_rsem,
    nar_ssem,
    nar_rsem,
):
    me = lax.axis_index("wide")
    core = lax.axis_index("narrow")
    tab_dev, vocab, emb_width = tables.shape
    cand = request.shape[1]
    part_rows = projected.shape[1]
    width = projected.shape[2] // SPLIT
    total = bias.shape[1]
    user_dim = user_weight.shape[1]
    req_dev = dense.shape[1]
    block = down.shape[1]
    column_block = up.shape[2]

    loads = {}
    for at, (name, source, target) in enumerate(
        (
            ("ids", ids_in, ids),
            ("proj", proj_in, proj),
            ("choice", choice_in, choice),
            ("rows", rows_in, rows),
            ("tables", tables_in, tables),
            ("dense", dense_in, dense.at[core]),
            ("request", request_in, request),
            ("user_weight", user_weight_in, user_weight),
            ("down", down_in, down.at[core]),
            ("deep", deep_in, deep_w.at[core]),
            ("up", up_in, up.at[core]),
            ("mid", mid_in, mid),
            ("bias", bias_in, bias),
            ("head_cross", head_cross_in, head_cross),
            ("head_deep", head_deep_in, head_deep),
        )
    ):
        loads[name] = pltpu.make_async_copy(source, target, local_sem.at[at])
        loads[name].start()

    barrier = pltpu.get_barrier_semaphore()

    plane_size = nw // PLANES
    my_plane = me // plane_size
    my_half = my_plane // 2
    planes = (2 - my_half, 3 - 3 * my_half, my_half * 2 + 1 - my_plane % 2, my_plane)

    def peer_at(order, i):
        return planes[order] * plane_size + (me + i + 1) % plane_size

    def each_peer(do):
        for order in range(PLANES):

            def step(i, carry, order=order):
                do(peer_at(order, i))
                return carry

            lax.fori_loop(0, plane_size - (order == PLANES - 1), step, 0, unroll=nw <= 16)

    def greet(peer):
        pl.semaphore_signal(
            barrier, inc=1, device_id={"wide": peer}, device_id_type=pl.DeviceIdType.MESH
        )

    each_peer(greet)
    for step in range(1, nn):
        pl.semaphore_signal(
            barrier,
            inc=1,
            device_id={"narrow": lax.rem(core + step, nn)},
            device_id_type=pl.DeviceIdType.MESH,
        )

    loads["ids"].wait()
    for o in range(nw):
        ids_send[o] = ids[o * tab_dev : (o + 1) * tab_dev, :]
    ids_recv[me] = ids_send[me]

    loads["proj"].wait()
    loads["choice"].wait()
    loads["tables"].wait()
    row_index = lax.broadcasted_iota(jnp.int32, (emb_width, width), 0)
    for t in range(tab_dev):
        kept = jnp.left_shift(jnp.full((1, 1), 32, jnp.int32), choice[:, t : t + 1])
        used = jnp.where(row_index < kept, proj[t].astype(F32), 0.0).astype(BF16)
        for h in range(SPLIT):
            projected[t, :, h * width : (h + 1) * width] = dot(
                tables[t, h * part_rows : (h + 1) * part_rows, :], used
            ).astype(BF16)

    pl.semaphore_wait(barrier, nw - 1 + nn - 1)

    def ids_copy(to, index):
        return pltpu.make_async_remote_copy(
            src_ref=ids_send.at[to],
            dst_ref=ids_recv.at[index],
            send_sem=ids_ssem.at[to],
            recv_sem=ids_rsem.at[index],
            device_id={"wide": to},
            device_id_type=pl.DeviceIdType.MESH,
        )

    def emb_copy(to, index):
        return pltpu.make_async_remote_copy(
            src_ref=emb_send.at[to],
            dst_ref=emb_recv.at[index],
            send_sem=emb_ssem.at[to],
            recv_sem=emb_rsem.at[index],
            device_id={"wide": to},
            device_id_type=pl.DeviceIdType.MESH,
        )

    def narrow_copy(kind, to, index):
        source, target = (
            (dense_in, dense),
            (down_in, down),
            (deep_in, deep_w),
            (up_in, up),
        )[kind]
        return pltpu.make_async_remote_copy(
            src_ref=source,
            dst_ref=target.at[index],
            send_sem=nar_ssem.at[kind, to],
            recv_sem=nar_rsem.at[kind, index],
            device_id={"narrow": to},
            device_id_type=pl.DeviceIdType.MESH,
        )

    each_peer(lambda peer: ids_copy(peer, me).start())
    for kind in range(4):
        for step in range(1, nn):
            narrow_copy(kind, lax.rem(core + step, nn), core).start()

    eye = lax.broadcasted_iota(jnp.int32, (cand, cand), 0) == lax.broadcasted_iota(
        jnp.int32, (cand, cand), 1
    )
    for name in ("request", "user_weight", "dense", "rows"):
        loads[name].wait()
    wanted = row_to_column(request[...].astype(F32), eye)
    for step in range(1, nn):
        narrow_copy(0, core, lax.rem(core + step, nn)).wait_recv()
    chosen = jnp.zeros((cand, dense.shape[2]), F32)
    for n in range(nn):
        for r in range(req_dev):
            chosen = jnp.where(
                wanted == float(n * req_dev + r), dense[n, r : r + 1, :].astype(F32), chosen
            )
    x0[:, :user_dim] = jax.nn.silu(dot(chosen.astype(BF16), user_weight[...])).astype(BF16)

    limit = rows[...].astype(F32)
    inverse = 1.0 / limit
    lane = lax.broadcasted_iota(jnp.int32, (cand, part_rows), 1).astype(F32)

    def look_up(order, group, last):
        highs = []
        for i in range(GROUP):
            peer = peer_at(order, group * GROUP + i)
            if not (last and i == GROUP - 1):
                ids_copy(me, peer).wait_recv()
            values = ids_recv[peer].astype(F32)
            for t in range(tab_dev):
                value = values[t : t + 1, :]
                most = limit[:, t : t + 1]
                index = value - jnp.floor(value * inverse[:, t : t + 1]) * most
                index = jnp.where(index < 0.0, index + most, index)
                index = jnp.where(index >= most, index - most, index)
                high = sum(
                    jnp.where(index >= float(h * part_rows), 1.0, 0.0) for h in range(1, SPLIT)
                )
                low_index = row_to_column(index - high * float(part_rows), eye)
                highs.append(row_to_column(high, eye))
                onehot[t, i * cand : (i + 1) * cand, :] = jnp.where(
                    low_index == lane, 1.0, 0.0
                ).astype(BF16)
        found = [dot(onehot[t], projected[t]) for t in range(tab_dev)]
        for i in range(GROUP):
            total_rows = jnp.zeros((cand, width), F32)
            for t in range(tab_dev):
                high = highs[i * tab_dev + t]
                for h in range(SPLIT):
                    piece = found[t][i * cand : (i + 1) * cand, h * width : (h + 1) * width]
                    total_rows = total_rows + jnp.where(high == float(h), piece, 0.0)
            part = total_rows.astype(BF16)
            if last and i == GROUP - 1:
                emb_recv[me] = part
            else:
                peer = peer_at(order, group * GROUP + i)
                emb_send[peer] = part
                emb_copy(peer, me).start()

    groups = plane_size // GROUP
    for order in range(PLANES):
        final = order == PLANES - 1

        def look_up_loop(group, carry, order=order):
            look_up(order, group, False)
            return carry

        if groups - final > 1:
            lax.fori_loop(0, groups - final, look_up_loop, 0)
        elif groups - final == 1:
            look_up(order, 0, False)
        if final:
            look_up(order, groups - 1, True)

    for name in ("down", "deep"):
        loads[name].wait()
    for kind in (1, 2):
        for step in range(1, nn):
            narrow_copy(kind, core, lax.rem(core + step, nn)).wait_recv()
    low = jnp.zeros((cand, down.shape[2]), F32)
    deep = jnp.zeros((cand, deep_w.shape[2]), F32)
    for n in range(user_dim // block):
        part = x0[:, n * block : (n + 1) * block]
        low = low + dot(part, down[n])
        deep = deep + dot(part, deep_w[n])

    for name in ("up", "mid", "bias", "head_cross", "head_deep"):
        loads[name].wait()
    for step in range(1, nn):
        narrow_copy(3, core, lax.rem(core + step, nn)).wait_recv()

    each_peer(lambda peer: emb_copy(me, peer).wait_recv())
    slots = (total - user_dim) // width
    for s in range(slots):
        item = emb_recv[s].astype(F32)
        for g in range(1, nw // slots):
            item = item + emb_recv[g * slots + s].astype(F32)
        x0[:, user_dim + s * width : user_dim + (s + 1) * width] = item.astype(BF16)
    for n in range(user_dim // block, total // block):
        part = x0[:, n * block : (n + 1) * block]
        low = low + dot(part, down[n])
        deep = deep + dot(part, deep_w[n])
    low = low.astype(BF16)
    deep = jax.nn.relu(deep).astype(BF16)
    score = jnp.zeros((cand, 1), F32)
    for n in range(nn):
        span = slice(n * column_block, (n + 1) * column_block)
        base = x0[:, span].astype(F32)
        out = (base * (dot(low, up[n]) + bias[:, span]) + base).astype(BF16)
        crossed[:, span] = out
        score = score + jnp.sum(out.astype(F32) * head_cross[:, span], axis=1, keepdims=True)
    hidden = jax.nn.relu(dot(deep, mid[...]))
    score = score + jnp.sum(hidden * head_deep[...], axis=1, keepdims=True)
    scores[...] = jnp.sum(jnp.where(eye, score, 0.0), axis=0, keepdims=True)

    def drain(peer):
        ids_copy(peer, me).wait_send()
        emb_copy(peer, me).wait_send()

    each_peer(drain)
    for kind in range(4):
        for step in range(1, nn):
            narrow_copy(kind, lax.rem(core + step, nn), core).wait_send()


def per_device(
    cand_ids,
    cand_request,
    tables,
    table_rows,
    width_choice,
    projections,
    user_dense,
    user_weight,
    cross_down,
    cross_up,
    cross_bias,
    deep_in,
    deep_mid,
    head_cross,
    head_deep,
):
    nw = lax.axis_size("wide")
    nn = lax.axis_size("narrow")
    cand = cand_request.shape[0]
    tab_dev, vocab, emb_width = tables.shape
    width = projections.shape[2]
    total = cross_bias.shape[0]
    operands = (
        cand_ids,
        cand_request.reshape(1, -1),
        tables,
        table_rows.reshape(1, -1),
        width_choice.reshape(1, -1),
        projections,
        user_dense,
        user_weight,
        cross_down,
        cross_up,
        cross_bias.reshape(1, -1),
        deep_in,
        deep_mid,
        head_cross.reshape(1, -1),
        head_deep.reshape(1, -1),
    )
    gathered = (6, 8, 9, 11)
    scratch = [
        pltpu.VMEM(((nn,) if at in gathered else ()) + a.shape, a.dtype)
        for at, a in enumerate(operands)
    ]
    scratch += [
        pltpu.VMEM((nw, tab_dev, cand), jnp.int32),
        pltpu.VMEM((nw, tab_dev, cand), jnp.int32),
        pltpu.VMEM((tab_dev, vocab // SPLIT, SPLIT * width), BF16),
        pltpu.VMEM((tab_dev, GROUP * cand, vocab // SPLIT), BF16),
        pltpu.VMEM((nw, cand, width), BF16),
        pltpu.VMEM((nw, cand, width), BF16),
        pltpu.VMEM((cand, total), BF16),
        pltpu.SemaphoreType.DMA((len(operands),)),
        pltpu.SemaphoreType.DMA((nw,)),
        pltpu.SemaphoreType.DMA((nw,)),
        pltpu.SemaphoreType.DMA((nw,)),
        pltpu.SemaphoreType.DMA((nw,)),
        pltpu.SemaphoreType.DMA((4, nn)),
        pltpu.SemaphoreType.DMA((4, nn)),
    ]
    crossed, scores = pl.pallas_call(
        functools.partial(kernel, nw, nn),
        out_shape=(pltpu.VMEM((cand, total), BF16), pltpu.VMEM((1, cand), F32)),
        in_specs=[pl.BlockSpec(memory_space=pl.ANY)] * len(operands),
        out_specs=(pl.BlockSpec(memory_space=pltpu.VMEM), pl.BlockSpec(memory_space=pltpu.VMEM)),
        scratch_shapes=scratch,
        compiler_params=pltpu.CompilerParams(
            collective_id=0, has_side_effects=True, vmem_limit_bytes=32 * 1024 * 1024
        ),
        name="score",
    )(*[pltpu.with_memory_space_constraint(a, pltpu.HBM) for a in operands])
    return crossed, scores.reshape(cand)


def solution(mesh):
    return jax.shard_map(
        per_device,
        mesh=mesh,
        in_specs=(
            P(None, ("wide", "narrow")),
            P(("wide", "narrow")),
            P("wide", None, None),
            P("wide"),
            P("wide"),
            P("wide", None, None),
            P(("wide", "narrow"), None),
            P(),
            P("narrow", None),
            P(None, "narrow"),
            P(),
            P("narrow", None),
            P(),
            P(),
            P(),
        ),
        out_specs=(P(("wide", "narrow"), None), P(("wide", "narrow"))),
        check_vma=False,
    )
```
